256 devices in a mesh: cache: 32 (over x, z), owner: 8 (over y, core).
Axes of the slice: x: 4, y: 4, z: 8, core: 2. Of those that a mesh axis runs over, the one named last changes fastest.
Arguments:
- cache: bfloat16 [32, 4, 128, 256], P('cache'), may hold values from -2.5 to 2.5
- backing: bfloat16 [32, 64, 128, 256], P('cache', 'owner'), may hold values from -2.5 to 2.5
- resident: int32 [32, 4], P('cache'), may hold values from 0 to 63, as said below
- promote: int32 [32, 2], P('cache'), may hold values from 0 to 63, as said below
- victim: int32 [32, 2], P('cache'), may hold values from 0 to 3, as said below
- lookups: int32 [2, 32768, 32, 8], P(None, 'owner', 'cache'), may hold values from 0 to 511
- route: int32 [2, 8, 4096], P(None, 'owner'), may hold values from 0 to 4095, each once within a row
- dcn_down: bfloat16 [8192, 128], P('cache'), may hold values from -0.0625 to 0.0625
- dcn_up: bfloat16 [128, 8192], P(None, 'cache'), may hold values from -0.5 to 0.5
- dcn_bias: float32 [8192], replicated, may hold values from -5 to 5
- mlp_in: bfloat16 [8192, 1024], P('cache'), may hold values from -0.0625 to 0.0625
- mlp_bias: float32 [1024], replicated, may hold values from -3 to 3
- mlp_out: float32 [1024], replicated, may hold values from -0.1875 to 0.1875
- out_bias: float32 [1], replicated, may hold values from -4 to 4
Outputs:
- scores: float32 [2, 8, 4096], P(None, 'owner', 'cache')
- new_cache: bfloat16 [32, 4, 128, 256], P('cache')
- new_backing: bfloat16 [32, 64, 128, 256], P('cache', 'owner')
The draws below stay inside these ranges and needn't reach their ends.
Inputs may be any that keep to these rules, and one draw needn't show every extreme that they name: `resident`: for each feature, 4 distinct backing blocks. `promote`: for each feature, 2 distinct backing blocks, none of them in that feature's resident; block k belongs to owner k // 8. `victim`: for each feature, 2 distinct slots. `route`: each batch and owner group holds every request index once.
All inputs are finite; a program needn't handle non-finite values.
Results may differ from the reference program's by a relative error of at most 0.004.
Values may be sent and summed in bfloat16 or wider, within the bound.
No kernel may reach another device: no remote copies, remote signals or barrier semaphores. Data moves between devices by JAX's collectives and lax.ppermute only.
A program may use at most 128 MiB of HBM per device.

```python
import math
import jax
import jax.numpy as jnp
import numpy as np
from jax import lax

E = 256
F = 32
HID = 1024
RANK = 128
BLOCK = 128
BAG = 8
BATCHES = 2
SLOTS = 4
OWN_BLK = 8
PROM = 2
D0 = 8192
BACK = 64
REQ_G = 4096
REQ = 32768
N_OWNER = 8


def common_plan(key):
    base_key = jax.random.fold_in(key, 11)

    def single(feature):
        feature_key = jax.random.fold_in(base_key, feature)
        first_key, second_key, third_key = jax.random.split(feature_key, 3)
        owners = BACK // OWN_BLK
        hot_owner = jax.random.randint(first_key, (), 0, owners)
        order_rank = jax.random.permutation(second_key, BACK).astype(jnp.int32)
        block_numbers = jnp.arange(BACK, dtype=jnp.int32)
        leaning = (feature % 2 == 0) & (block_numbers // OWN_BLK == hot_owner)
        promote_score = order_rank - jnp.where(leaning, BACK, 0)
        promoted = jnp.argsort(promote_score, stable=True)[:PROM].astype(jnp.int32)
        chosen_set = jnp.any(block_numbers[:, None] == promoted[None, :], axis=1)
        resident = jnp.argsort(order_rank + jnp.where(chosen_set, 2 * BACK, 0), stable=True)[:SLOTS].astype(jnp.int32)
        victims = jax.random.permutation(third_key, SLOTS)[:PROM].astype(jnp.int32)
        return (resident, promoted, victims)
    return jax.vmap(single)(jnp.arange(F, dtype=jnp.int32))


def draw_resident(key, part):
    return common_plan(key)[0]


def draw_promote(key, part):
    return common_plan(key)[1]


def draw_victim(key, part):
    return common_plan(key)[2]


def place_ends(entries, own_key, low, high):
    dims = entries.shape
    place = [jax.random.randint(jax.random.fold_in(own_key, axis), (), 0, dims[axis]) for axis in range(len(dims))]
    entries = entries.at[tuple(place)].set(low)
    longest = dims.index(max(dims))
    place[longest] = (place[longest] + 1) % dims[longest]
    return entries.at[tuple(place)].set(high)


def levels(rng, extent, shards, low, largest):
    def one(position, parts):
        draws = jax.random.uniform(jax.random.fold_in(jax.random.fold_in(rng, 6), position), (parts,), jnp.float32, low / len(shards), largest / len(shards))
        return jnp.repeat(jnp.exp(draws), extent[position] // parts).reshape((-1,) + (1,) * (len(extent) - position - 1))

    gain = one(*shards[0])
    for cut in shards[1:]:
        gain = gain * one(*cut)
    return gain


def rank_bounds(count, lean):
    portions = [(1 << 20) // math.isqrt(rank ** lean) + 1 for rank in range(1, count + 1)]
    scale = 1 + sum(portions) // (1 << 30)
    return np.cumsum(np.array([max(1, weight // scale) for weight in portions]))


def ranked_ids(rng, shape, amount, slope):
    grid = rank_bounds(amount, slope)
    lot = jax.random.randint(jax.random.fold_in(rng, 1), shape, 0, int(grid[amount - 1]))
    grade = jnp.searchsorted(jnp.asarray(grid, jnp.int32), lot, side="right")
    return jax.random.permutation(jax.random.fold_in(rng, 2), amount)[grade].astype(jnp.int32)


def scatter_about(own_key, shape, width, most, cuts=(), kind=jnp.bfloat16):
    array = width * jax.random.normal(own_key, shape, jnp.float32)
    if cuts:
        array = array * levels(own_key, shape, cuts, -0.22, 0.18)
    return jnp.clip(array, -most, most).astype(kind)


def setup_inputs(seed: int = 0) -> dict:
    key_of = jax.random.split(jax.random.key(seed), 15)
    cache = scatter_about(key_of[0], (F, SLOTS, BLOCK, E), 0.35, 2.5, ((0, 32),))
    backing = scatter_about(key_of[1], (F, BACK, BLOCK, E), 0.35, 2.5, ((0, 32), (1, 8)))
    resident = draw_resident(jax.random.fold_in(key_of[14], 71), 0)
    promote = draw_promote(jax.random.fold_in(key_of[14], 71), 0)
    victim = draw_victim(jax.random.fold_in(key_of[14], 71), 0)
    lookups = place_ends(ranked_ids(key_of[5], (BATCHES, REQ, F, BAG), SLOTS * BLOCK, 2), jax.random.fold_in(key_of[5], 3), 0, (SLOTS * BLOCK) - 1).astype(jnp.int32)
    route = jax.vmap(lambda own: jax.random.permutation(own, REQ_G))(jax.random.split(key_of[6], BATCHES * N_OWNER)).reshape((BATCHES, N_OWNER, REQ_G)).astype(jnp.int32)
    dcn_down = scatter_about(key_of[7], (D0, RANK), D0 ** -0.5, 0.0625, ((0, 32),))
    dcn_up = scatter_about(key_of[8], (RANK, D0), RANK ** -0.5, 0.5, ((1, 32),))
    dcn_bias = scatter_about(key_of[9], (D0,), 1.0, 5.0, (), jnp.float32)
    mlp_in = scatter_about(key_of[10], (D0, HID), D0 ** -0.5, 0.0625, ((0, 32),))
    mlp_bias = scatter_about(key_of[11], (HID,), 0.5, 3.0, (), jnp.float32)
    mlp_out = scatter_about(key_of[12], (HID,), HID ** -0.5, 0.1875, (), jnp.float32)
    out_bias = scatter_about(key_of[13], (1,), 1.0, 4.0, (), jnp.float32)
    return dict(cache=cache, backing=backing, resident=resident, promote=promote, victim=victim, lookups=lookups, route=route, dcn_down=dcn_down, dcn_up=dcn_up, dcn_bias=dcn_bias, mlp_in=mlp_in, mlp_bias=mlp_bias, mlp_out=mlp_out, out_bias=out_bias)


def take_rows(table, wanted):
    return jax.vmap(lambda rows, chosen: rows[chosen])(table, wanted)


def dense_rows(features, dcn_down, dcn_up, dcn_bias, mlp_in, mlp_bias, mlp_out, out_bias):
    low = jnp.dot(features, dcn_down, preferred_element_type=jnp.float32).astype(jnp.bfloat16)
    gate = jnp.dot(low, dcn_up, preferred_element_type=jnp.float32) + dcn_bias
    crossed = (features * gate + features).astype(jnp.bfloat16)
    hidden = jnp.maximum(jnp.dot(crossed, mlp_in, preferred_element_type=jnp.float32) + mlp_bias, 0.0)
    return jnp.sum(hidden * mlp_out, axis=-1) + out_bias[0]


def reference(cache, backing, resident, promote, victim, lookups, route, dcn_down, dcn_up, dcn_bias, mlp_in, mlp_bias, mlp_out, out_bias):
    fetched = take_rows(backing, promote)
    evicted = take_rows(cache, victim)
    leaving = take_rows(resident, victim)
    slot_numbers = jnp.arange(SLOTS, dtype=jnp.int32)
    block_numbers = jnp.arange(BACK, dtype=jnp.int32)
    new_cache = cache
    new_backing = backing
    for column in range(PROM):
        slot_hit = victim[:, column][:, None] == slot_numbers[None, :]
        new_cache = jnp.where(slot_hit[:, :, None, None], fetched[:, column][:, None], new_cache)
        block_hit = leaving[:, column][:, None] == block_numbers[None, :]
        new_backing = jnp.where(block_hit[:, :, None, None], evicted[:, column][:, None], new_backing)
    table = new_cache.reshape(F, SLOTS * BLOCK, E)

    def pool_feature(pair):
        rows, wanted = pair
        return jnp.sum(rows[wanted].astype(jnp.float32), axis=1).astype(jnp.bfloat16)

    step = min(1024, REQ)
    results = []
    for batch_turn in range(BATCHES):
        pooled = lax.map(pool_feature, (table, jnp.transpose(lookups[batch_turn], (1, 0, 2))))
        pooled = jnp.transpose(pooled, (1, 0, 2))
        offsets = (jnp.arange(N_OWNER, dtype=jnp.int32) * REQ_G)[:, None]
        order = (route[batch_turn] + offsets).reshape(-1)
        features = pooled[order].reshape(REQ // step, step, D0)
        scored = lax.map(lambda block_rows: dense_rows(block_rows, dcn_down, dcn_up, dcn_bias, mlp_in, mlp_bias, mlp_out, out_bias), features)
        results.append(scored.reshape(N_OWNER, REQ_G))
    scores = jnp.stack(results)
    return scores, new_cache, new_backing
```

```python
import jax
import jax.numpy as jnp
from jax import lax
from jax.experimental import pallas as pl
from jax.experimental.pallas import tpu as pltpu
from jax.sharding import Mesh, PartitionSpec as P

BF = jnp.bfloat16
F32 = jnp.float32
NX, NZ, NY, NC = 4, 8, 4, 2
SLOTS, BLOCK, E = 4, 128, 256
HID, RANK = 1024, 128
LANE = 128


SMEM = pl.BlockSpec(memory_space=pltpu.SMEM)
VMEM = pl.BlockSpec(memory_space=pltpu.VMEM)
ANY = pl.BlockSpec(memory_space=pl.ANY)


def near(*vs):
    return [pltpu.with_memory_space_constraint(v, pltpu.VMEM) for v in vs]


def kernel(body, out_shape, in_specs, out_specs, scratch=(), flops=0, limit=16):
    return pl.pallas_call(
        body,
        out_shape=out_shape,
        in_specs=in_specs,
        out_specs=out_specs,
        scratch_shapes=list(scratch),
        compiler_params=pltpu.CompilerParams(vmem_limit_bytes=limit * 1024 * 1024),
        cost_estimate=pl.CostEstimate(flops=flops, bytes_accessed=0, transcendentals=0),
    )


def bf(*shape):
    return jax.ShapeDtypeStruct(shape, BF)


def fetch_body(promote, victim, backing, out, blocks, sems):
    count = backing.shape[0]
    base = (lax.axis_index("y") * NC + lax.axis_index("c")) * count
    copies = []
    for k in range(2):
        at = jnp.clip(promote[0, k] - base, 0, count - 1)
        copies.append(pltpu.make_async_copy(backing.at[at], blocks.at[k], sems.at[k]))
    for copy in copies:
        copy.start()
    out[...] = jnp.zeros(out.shape, BF)
    for copy in copies:
        copy.wait()
    for k in range(2):
        local = promote[0, k] - base

        @pl.when((local >= 0) & (local < count))
        def _():
            s = victim[0, k]
            out[2 * s] = blocks[k, :, :LANE]
            out[2 * s + 1] = blocks[k, :, LANE:]


def fetch(promote, victim, backing):
    return kernel(
        fetch_body, bf(NY * NC, BLOCK, LANE), [SMEM, SMEM, ANY], VMEM,
        [pltpu.VMEM((2, BLOCK, E), BF), pltpu.SemaphoreType.DMA((2,))],
    )(promote, victim, pltpu.with_memory_space_constraint(backing, pltpu.HBM))


def piece_body(victim, arrived, cache, factors, sent, out):
    s = lax.axis_index("y")
    c = lax.axis_index("c")
    total = arrived[0]
    for i in range(1, NY * NC):
        total = total + arrived[i]
    block = cache[s]
    kept = jnp.where(c == 0, block[:, :LANE], block[:, LANE:])
    evicted = (victim[0, 0] == s) | (victim[0, 1] == s)
    piece = jnp.where(evicted, total, kept).T
    for i in range(NZ):
        out[i, :LANE, :] = piece
        out[i, LANE:192, :] = factors[...]
        out[i, 192:, :] = sent[i]


def make_piece(victim, arrived, cache, factors, sent):
    return kernel(
        piece_body, bf(NZ, 256, BLOCK), [SMEM] + [VMEM] * 4, VMEM
    )(victim, *near(arrived, cache, factors, sent))


def back_body(resident, victim, cache, backing, out):
    base = (lax.axis_index("y") * NC + lax.axis_index("c")) * backing.shape[0]
    out[...] = backing[...]
    for k in range(2):
        v = victim[0, k]
        local = resident[0, v] - base

        @pl.when((local >= 0) & (local < backing.shape[0]))
        def _():
            out[local] = cache[v]


def write_back(resident, victim, cache, backing):
    return kernel(
        back_body, jax.ShapeDtypeStruct(backing.shape, BF), [SMEM, SMEM, VMEM, VMEM], VMEM
    )(resident, victim, cache, backing)


def route_body(lookups, route, out):
    batches, bag, count = lookups.shape
    tiles = count // LANE

    def one(t, _):
        q = t // NZ
        z = t % NZ
        parts = []
        for b in range(batches):
            row = jnp.broadcast_to(route[b, pl.ds(t, 1), :], (bag, LANE))
            lane = row & (LANE - 1)
            tile = row >> 7
            got = jnp.zeros((bag, LANE), jnp.int32)
            for v in range(tiles):
                cand = jnp.take_along_axis(
                    lookups[b, :, v * LANE : (v + 1) * LANE], lane, axis=1, mode="promise_in_bounds"
                )
                got = jnp.where(tile == v, cand, got)
            parts.append(got)
        both = (jnp.concatenate(parts, axis=0) - 256).astype(F32).astype(BF)
        out[z, pl.ds(pl.multiple_of(q * 16, 16), 16), :] = both
        return 0

    lax.fori_loop(0, NX * NZ, one, 0)


def route_lookups(lookups, route):
    return kernel(route_body, bf(NZ, 64, LANE), [VMEM, VMEM], VMEM, flops=1 << 22)(lookups, route)


def weights_body(down, up, mlp, factors, top, scratch):
    o = lax.axis_index("y") * NC + lax.axis_index("c")
    rows = RANK // (NY * NC)
    at = pl.multiple_of(o * rows, rows)
    scratch[...] = down[...].T
    piece = jnp.concatenate([scratch[pl.ds(at, rows), :], up[pl.ds(at, rows), :]], axis=0)
    factors[0:32, :] = piece[:, :LANE]
    factors[32:64, :] = piece[:, LANE:]
    top[...] = mlp[:, pl.ds(pl.multiple_of(o * LANE, LANE), LANE)].T


def own_weights(down, up, mlp):
    return kernel(
        weights_body, [bf(64, LANE), bf(LANE, E)], [VMEM] * 3, [VMEM] * 2, [pltpu.VMEM((RANK, E), BF)]
    )(down, up, mlp)


def factor(tables, i, start):
    rows = [
        jnp.concatenate([t[i, start : start + 16, :], t[i, start + 32 : start + 48, :]], axis=1)
        for t in tables
    ]
    return jnp.concatenate(rows, axis=0)


def far(*vs):
    return [pltpu.with_memory_space_constraint(v, pltpu.HBM) for v in vs]


def load(sources, holds, sems):
    waits = []
    for i in range(NZ):
        step = []
        for n, (source, hold) in enumerate(zip(sources, holds)):
            copy = pltpu.make_async_copy(source.at[i], hold.at[i], sems.at[n, i])
            copy.start()
            step.append(copy)
        waits.append(step)
    return waits


def pool_step(batch, i, table, down, lookups, codes, hold):
    for q in range(NX):
        wanted = lookups[i, q * 16 + batch * 8 : q * 16 + batch * 8 + 8, :]
        rows = [jnp.broadcast_to(wanted[l : l + 1, :], (BLOCK, LANE)) for l in range(8)]
        for r in range(NY):
            total = jnp.where(rows[0] == codes[r], jnp.ones((), BF), jnp.zeros((), BF))
            for l in range(1, 8):
                total = total + jnp.where(rows[l] == codes[r], jnp.ones((), BF), jnp.zeros((), BF))
            hold[r * BLOCK : (r + 1) * BLOCK, q * LANE : (q + 1) * LANE] = total
    pooled = jnp.dot(table, hold[...], preferred_element_type=F32).astype(BF)
    return pooled, jnp.dot(down, pooled, preferred_element_type=F32)


def slot_codes():
    y = lax.axis_index("y")
    line = lax.broadcasted_iota(jnp.int32, (BLOCK, LANE), 0)
    return [(line + (((y + r) % NY) * BLOCK - 256)).astype(F32).astype(BF) for r in range(NY)]


def pool0_body(lookups, *refs):
    tables = refs[0:8]
    x0_out, low_out, table_out, factor_out, new_cache = refs[8:13]
    counts, x0, whole_table, factors, sems = refs[13:]
    y = lax.axis_index("y")
    c = lax.axis_index("c")
    codes = slot_codes()
    low = None
    copies = []
    for i in range(NZ):
        mine = jnp.concatenate([t[i, :LANE, :] for t in tables[:4]], axis=1)
        theirs = jnp.concatenate([t[i, :LANE, :] for t in tables[4:]], axis=1)
        table = jnp.concatenate([jnp.where(c == 0, mine, theirs), jnp.where(c == 0, theirs, mine)], axis=0)
        whole_table[i] = table
        down = factor(tables, i, LANE)
        factors[i, :RANK, :] = down
        factors[i, RANK:, :] = factor(tables, i, LANE + 16)

        @pl.when(lax.axis_index("z") == i)
        def _():
            for r in range(NY):
                new_cache[(y + r) % NY] = table[:, r * BLOCK : (r + 1) * BLOCK].T

        pooled, part = pool_step(0, i, table, down, lookups, codes, counts.at[i % 2])
        x0[i] = pooled
        low = part if low is None else low + part
        for n, (source, out) in enumerate(((x0, x0_out), (whole_table, table_out), (factors, factor_out))):
            copy = pltpu.make_async_copy(source.at[i], out.at[i], sems.at[n, i])
            copy.start()
            copies.append(copy)
    low_out[...] = low
    for copy in copies:
        copy.wait()


MANY = NX * LANE


def pool0(lookups, tables):
    return kernel(
        pool0_body,
        [pltpu.HBM((NZ, E, MANY), BF), jax.ShapeDtypeStruct((RANK, MANY), F32), pltpu.HBM((NZ, E, SLOTS * BLOCK), BF),
         pltpu.HBM((NZ, 2 * RANK, E), BF), bf(SLOTS, BLOCK, E)],
        [VMEM] * 9, [ANY, VMEM, ANY, ANY, VMEM],
        [pltpu.VMEM((2, SLOTS * BLOCK, MANY), BF), pltpu.VMEM((NZ, E, MANY), BF), pltpu.VMEM((NZ, E, SLOTS * BLOCK), BF),
         pltpu.VMEM((NZ, 2 * RANK, E), BF), pltpu.SemaphoreType.DMA((3, NZ))],
        flops=1 << 32, limit=24,
    )(*near(lookups, *tables))


def pool1_body(lookups, table_in, factor_in, x0_out, low_out, counts, x0, tables, factors, sems, out_sems):
    codes = slot_codes()
    low = None
    copies = []
    waits = load((table_in, factor_in), (tables, factors), sems)
    for i in range(NZ):
        for copy in waits[i]:
            copy.wait()
        pooled, part = pool_step(1, i, tables[i], factors[i, :RANK, :], lookups, codes, counts.at[i % 2])
        x0[i] = pooled
        low = part if low is None else low + part
        copy = pltpu.make_async_copy(x0.at[i], x0_out.at[i], out_sems.at[i])
        copy.start()
        copies.append(copy)
    low_out[...] = low
    for copy in copies:
        copy.wait()


def pool1(lookups, table, factors):
    return kernel(
        pool1_body, [pltpu.HBM((NZ, E, MANY), BF), jax.ShapeDtypeStruct((RANK, MANY), F32)],
        [VMEM, ANY, ANY], [ANY, VMEM],
        [pltpu.VMEM((2, SLOTS * BLOCK, MANY), BF), pltpu.VMEM((NZ, E, MANY), BF), pltpu.VMEM((NZ, E, SLOTS * BLOCK), BF),
         pltpu.VMEM((NZ, 2 * RANK, E), BF), pltpu.SemaphoreType.DMA((2, NZ)), pltpu.SemaphoreType.DMA((NZ,))],
        flops=1 << 32, limit=24,
    )(*near(lookups), *far(table, factors))


def gate_body(l0, l1, l2, l3, bias, x0_in, factor_in, x1_out, x0, factors, sems, out_sems):
    x = lax.axis_index("x")
    waits = load((x0_in, factor_in), (x0, factors), sems)
    low = (l0[...] + l1[...] + l2[...] + l3[...]).astype(BF)
    columns = bias[pl.ds(pl.multiple_of(x * NZ, NZ), NZ), :].T
    copies = []
    for i in range(NZ):
        for copy in waits[i]:
            copy.wait()
        gate = lax.dot_general(factors[i, RANK:, :], low, (((0,), (0,)), ((), ())), preferred_element_type=F32)
        gate = gate + columns[:, i : i + 1]
        features = x0[i].astype(F32)
        x0[i] = (features * gate + features).astype(BF)
        copy = pltpu.make_async_copy(x0.at[i], x1_out.at[i], out_sems.at[i])
        copy.start()
        copies.append(copy)
    for copy in copies:
        copy.wait()


def gate(lows, bias, x0, factors):
    return kernel(
        gate_body, pltpu.HBM((NZ, E, MANY), BF), [VMEM] * 5 + [ANY] * 2, ANY,
        [pltpu.VMEM((NZ, E, MANY), BF), pltpu.VMEM((NZ, 2 * RANK, E), BF),
         pltpu.SemaphoreType.DMA((2, NZ)), pltpu.SemaphoreType.DMA((NZ,))],
        flops=1 << 31,
    )(*near(*lows, bias), *far(x0, factors))


def top_body(x1_0, x1_1, t0, t1, t2, t3, *refs):
    outs = refs[0:4]
    weights, crossed, hold, sems = refs[4:]
    x = lax.axis_index("x")
    copies = []
    for b, source in enumerate((x1_0, x1_1)):
        step = []
        for i in range(NZ):
            copy = pltpu.make_async_copy(source.at[i], crossed.at[b, pl.ds(i * E, E), :], sems.at[b, i])
            copy.start()
            step.append(copy)
        copies.append(step)
    for i in range(NZ):
        for j, t in enumerate((t0, t1, t2, t3)):
            weights[j * LANE : (j + 1) * LANE, i * E : (i + 1) * E] = t[i]
    for b in range(2):
        for copy in copies[b]:
            copy.wait()
        part = jnp.dot(weights[...], crossed[b], preferred_element_type=F32).astype(BF)
        for q in range(NX):
            hold[q, :, b * LANE : (b + 1) * LANE] = part[:, q * LANE : (q + 1) * LANE]
    for r in range(NX):
        outs[r][...] = hold[(x + r) % NX]


def top_half(x1, tops):
    return kernel(
        top_body, [bf(HID // 2, 2 * LANE)] * NX, [ANY] * 2 + [VMEM] * 4, [VMEM] * NX,
        [pltpu.VMEM((HID // 2, NZ * E), BF), pltpu.VMEM((2, NZ * E, MANY), BF),
         pltpu.VMEM((NX, HID // 2, 2 * LANE), BF), pltpu.SemaphoreType.DMA((2, NZ))],
        flops=1 << 32, limit=24,
    )(*far(*x1), *near(*tops))


def score_body(mlp_bias, mlp_out, out_bias, *refs):
    hs = refs[0:8]
    out, rows = refs[8:]
    y = lax.axis_index("y")
    c = lax.axis_index("c")
    for j in range(8):
        o = ((y + j % 4) % NY) * NC + (c + j // 4) % NC
        rows[j : j + 1, :] = mlp_bias[pl.ds(o, 1), :]
        rows[8 + j : 9 + j, :] = mlp_out[pl.ds(o, 1), :]
    columns = rows[...].T
    total = jnp.zeros((LANE, 2 * LANE), F32)
    for j in range(8):
        before = columns[:, j : j + 1]
        for h in hs[4 * (j // 4) : 4 * (j // 4) + 4]:
            before = before + h[(j % 4) * LANE : (j % 4 + 1) * LANE, :].astype(F32)
        total = total + jnp.maximum(before, 0.0) * columns[:, 8 + j : 9 + j]
    total = jnp.sum(total, axis=0, keepdims=True) + out_bias[0]
    for b in range(2):
        out[b : b + 1, :] = total[:, b * LANE : (b + 1) * LANE]


def score(mlp_bias, mlp_out, out_bias, ha, hb):
    return kernel(
        score_body, jax.ShapeDtypeStruct((2, LANE), F32), [VMEM, VMEM, SMEM] + [VMEM] * 8, VMEM,
        [pltpu.VMEM((16, LANE), F32)],
    )(mlp_bias, mlp_out, out_bias, *near(*ha, *hb))


def shift(v, axis, size, k):
    return lax.ppermute(v, axis, [(i, (i + k) % size) for i in range(size)])


def spread(v, axis, size):
    out = [v]
    for k in range(1, size):
        out.append(shift(v, axis, size, size - k))
    return out


def deal(parts):
    out = [parts[0]]
    for k in range(1, NX):
        out.append(shift(parts[k], "x", NX, k))
    return out


def exchange(v, axis):
    return lax.all_to_all(v, axis, 0, 0, tiled=True)


def swaps(vs):
    return [shift(v, "c", NC, 1) for v in vs]


def tie(v, *others):
    return lax.optimization_barrier((v, *others))[0]


def on_device(
    cache, backing, resident, promote, victim, lookups, route,
    dcn_down, dcn_up, dcn_bias, mlp_in, mlp_bias, mlp_out, out_bias,
):
    cache = cache[0]
    backing = backing[0]
    bias = dcn_bias.reshape(-1, E)
    outgoing = fetch(promote, victim, backing)
    arrived = exchange(outgoing, ("y", "c"))
    wanted = jnp.transpose(lookups[:, :, 0, :], (0, 2, 1))
    factors, top = own_weights(dcn_down, dcn_up, mlp_in)
    sent = route_lookups(wanted, route[:, 0].reshape(2, -1, LANE))
    piece = make_piece(victim, arrived, cache, factors, sent)
    mixed = exchange(piece, "z")
    own = spread(mixed[:, :192, :], "y", NY)
    mixed = mixed[:, 192:, :]
    tops = jnp.broadcast_to(tie(top, mixed)[None], (NZ, *top.shape))
    tops = exchange(tops, "z")
    tables = own + swaps(own)
    own = spread(tops, "y", NY)
    other = swaps(own)
    x00, low0, table, factors, new_cache = pool0(mixed, tables)
    lows0 = spread(low0, "x", NX)
    x01, low1 = pool1(tie(mixed, low0), table, factors)
    lows1 = spread(low1, "x", NX)
    x10 = gate(lows0, bias, tie(x00, low1), factors)
    x11 = gate(lows1, bias, x01, factors)
    ha = top_half((x10, x11), own)
    ra = deal(ha)
    hb = top_half((x10, tie(x11, ha[0])), other)
    rb = deal(hb)
    new_backing = write_back(resident, victim, cache, backing)
    scores = score(mlp_bias.reshape(8, LANE), mlp_out.reshape(8, LANE), out_bias, ra, rb)
    return scores[:, None, :], new_cache[None], new_backing[None]


def solution(mesh):
    fine = Mesh(mesh.devices.reshape(NX, NZ, NY, NC), ("x", "z", "y", "c"))
    ca, ow = ("x", "z"), ("y", "c")
    in_specs = (
        P(ca, None, None, None),
        P(ca, ow, None, None),
        P(ca, None),
        P(ca, None),
        P(ca, None),
        P(None, ow, ca, None),
        P(None, ow, None),
        P(ca, None),
        P(None, ca),
        P(),
        P(ca, None),
        P(),
        P(),
        P(),
    )
    out_specs = (
        P(None, ow, ca),
        P(ca, None, None, None),
        P(ca, ow, None, None),
    )
    return jax.shard_map(
        on_device, mesh=fine, in_specs=in_specs, out_specs=out_specs, check_vma=False
    )
```

```python
import jax
import jax.numpy as jnp
from jax import lax
from jax.experimental import pallas as pl
from jax.experimental.pallas import tpu as pltpu
from jax.sharding import Mesh, PartitionSpec as P

BF = jnp.bfloat16
F32 = jnp.float32
NX, NZ, NY, NC = 4, 8, 4, 2
SLOTS, BLOCK, E = 4, 128, 256
HID, RANK = 1024, 128
LANE = 128


SMEM = pl.BlockSpec(memory_space=pltpu.SMEM)
VMEM = pl.BlockSpec(memory_space=pltpu.VMEM)
ANY = pl.BlockSpec(memory_space=pl.ANY)


def near(*vs):
    return [pltpu.with_memory_space_constraint(v, pltpu.VMEM) for v in vs]


def far(*vs):
    return [pltpu.with_memory_space_constraint(v, pltpu.HBM) for v in vs]


def kernel(body, out_shape, in_specs, out_specs, scratch=(), flops=0, limit=16):
    return pl.pallas_call(
        body,
        out_shape=out_shape,
        in_specs=in_specs,
        out_specs=out_specs,
        scratch_shapes=list(scratch),
        compiler_params=pltpu.CompilerParams(vmem_limit_bytes=limit * 1024 * 1024),
        cost_estimate=pl.CostEstimate(flops=flops, bytes_accessed=0, transcendentals=0),
    )


def bf(*shape):
    return jax.ShapeDtypeStruct(shape, BF)


def fetch_body(promote_in, victim_in, backing, out, promote, victim, blocks, sems):
    count = backing.shape[0]
    base = (lax.axis_index("y") * NC + lax.axis_index("c")) * count
    small = [
        pltpu.make_async_copy(promote_in, promote, sems.at[2]),
        pltpu.make_async_copy(victim_in, victim, sems.at[3]),
    ]
    for copy in small:
        copy.start()
    out[...] = jnp.zeros(out.shape, BF)
    for copy in small:
        copy.wait()
    copies = []
    for k in range(2):
        at = jnp.clip(promote[0, k] - base, 0, count - 1)
        copies.append(pltpu.make_async_copy(backing.at[at], blocks.at[k], sems.at[k]))
    for copy in copies:
        copy.start()
    for copy in copies:
        copy.wait()
    for k in range(2):
        local = promote[0, k] - base

        @pl.when((local >= 0) & (local < count))
        def _():
            s = victim[0, k]
            out[2 * s] = blocks[k, :, :LANE]
            out[2 * s + 1] = blocks[k, :, LANE:]


def fetch(promote, victim, backing):
    return kernel(
        fetch_body, bf(NY * NC, BLOCK, LANE), [ANY] * 3, VMEM,
        [pltpu.SMEM((1, 2), jnp.int32), pltpu.SMEM((1, 2), jnp.int32),
         pltpu.VMEM((2, BLOCK, E), BF), pltpu.SemaphoreType.DMA((4,))],
    )(*far(promote, victim, backing))


def piece_body(victim, arrived, cache, factors, sent, out):
    s = lax.axis_index("y")
    c = lax.axis_index("c")
    total = arrived[0]
    for i in range(1, NY * NC):
        total = total + arrived[i]
    block = cache[s]
    kept = jnp.where(c == 0, block[:, :LANE], block[:, LANE:])
    evicted = (victim[0, 0] == s) | (victim[0, 1] == s)
    piece = jnp.where(evicted, total, kept).T
    for i in range(NZ):
        out[i, :LANE, :] = piece
        out[i, LANE:160, :] = factors[...]
        out[i, 160:, :] = sent[i]


def make_piece(victim, arrived, cache, factors, sent):
    return kernel(
        piece_body, bf(NZ, 224, BLOCK), [SMEM] + [VMEM] * 4, VMEM
    )(victim, *near(arrived, cache, factors, sent))


def back_body(resident, victim, cache, backing, out):
    base = (lax.axis_index("y") * NC + lax.axis_index("c")) * backing.shape[0]
    out[...] = backing[...]
    for k in range(2):
        v = victim[0, k]
        local = resident[0, v] - base

        @pl.when((local >= 0) & (local < backing.shape[0]))
        def _():
            out[local] = cache[v]


def write_back(resident, victim, cache, backing):
    return kernel(
        back_body, jax.ShapeDtypeStruct(backing.shape, BF), [SMEM, SMEM, VMEM, VMEM], VMEM
    )(resident, victim, cache, backing)


def route_body(lookups_in, route_in, down_in, out, factors, lookups, route, down, scratch, sems):
    copies = [
        pltpu.make_async_copy(source, hold, sems.at[n])
        for n, (source, hold) in enumerate(((down_in, down), (route_in, route), (lookups_in, lookups)))
    ]
    for copy in copies:
        copy.start()
    copies[0].wait()
    o = lax.axis_index("y") * NC + lax.axis_index("c")
    rows = RANK // (NY * NC)
    scratch[...] = down[...].T
    piece = scratch[pl.ds(pl.multiple_of(o * rows, rows), rows), :]
    factors[0:16, :] = piece[:, :LANE]
    factors[16:32, :] = piece[:, LANE:]
    copies[1].wait()
    copies[2].wait()
    batches, bag, count = lookups.shape
    tiles = count // LANE

    def one(z, _):
        for q in range(NX):
            parts = []
            for b in range(batches):
                row = jnp.broadcast_to(route[b, pl.ds(q * NZ + z, 1), :], (bag, LANE))
                lane = row & (LANE - 1)
                tile = row >> 7
                got = jnp.zeros((bag, LANE), jnp.int32)
                for v in range(tiles):
                    cand = jnp.take_along_axis(
                        lookups[b, :, v * LANE : (v + 1) * LANE], lane, axis=1, mode="promise_in_bounds"
                    )
                    got = jnp.where(tile == v, cand, got)
                parts.append(got)
            both = (jnp.concatenate(parts, axis=0) - 256).astype(F32).astype(BF)
            out[z, q * 16 : q * 16 + 16, :] = both
        return 0

    lax.fori_loop(0, NZ, one, 0)


def route_lookups(lookups, route, down):
    return kernel(
        route_body, [bf(NZ, 64, LANE), bf(32, LANE)], [ANY] * 3, [VMEM] * 2,
        [pltpu.VMEM(lookups.shape, jnp.int32), pltpu.VMEM(route.shape, jnp.int32), pltpu.VMEM(down.shape, BF),
         pltpu.VMEM((RANK, E), BF), pltpu.SemaphoreType.DMA((3,))],
        flops=1 << 22,
    )(*far(lookups, route, down))


def own_body(up, mlp, out):
    o = lax.axis_index("y") * NC + lax.axis_index("c")
    rows = RANK // (NY * NC)
    out[:LANE, :] = mlp[:, pl.ds(pl.multiple_of(o * LANE, LANE), LANE)].T
    out[LANE:, :] = up[pl.ds(pl.multiple_of(o * rows, rows), rows), :]


def own_weights(up, mlp):
    return kernel(own_body, bf(LANE + 16, E), [VMEM] * 2, VMEM)(up, mlp)


def stack_body(*refs):
    out = refs[-1]
    z = lax.axis_index("z")
    for k in range(NZ):
        out[(z + k) % NZ] = refs[k][...]


def stacked(parts):
    return kernel(stack_body, bf(NZ, LANE + 16, E), [VMEM] * NZ, VMEM)(*near(*parts))


def factor(tables, i):
    rows = [jnp.concatenate([t[i, LANE : LANE + 16, :], t[i, LANE + 16 :, :]], axis=1) for t in tables]
    return jnp.concatenate(rows, axis=0)


def load(sources, holds, sems):
    waits = []
    for i in range(NZ):
        step = []
        for n, (source, hold) in enumerate(zip(sources, holds)):
            copy = pltpu.make_async_copy(source.at[i], hold.at[i], sems.at[n, i])
            copy.start()
            step.append(copy)
        waits.append(step)
    return waits


def pool_step(batch, i, table, down, lookups, hold):
    y = lax.axis_index("y")
    line = lax.broadcasted_iota(jnp.int32, (BLOCK, LANE), 0).astype(F32).astype(BF)
    none = jnp.zeros((), BF)
    for q in range(NX):
        wanted = lookups[i, q * 16 + batch * 8 : q * 16 + batch * 8 + 8, :]
        wanted = wanted.astype(F32).astype(jnp.int32) + 256
        slot = ((wanted >> 7) + (NY - y)) & 3
        weight = jnp.where((slot & 1) == 1, 16.0, 1.0)
        row = (wanted & (BLOCK - 1)).astype(F32).astype(BF)
        lower = jnp.where(slot < 2, weight, 0.0).astype(BF)
        upper = jnp.where(slot < 2, 0.0, weight).astype(BF)
        sums = [None, None]
        for l in range(8):
            hit = jnp.broadcast_to(row[l : l + 1, :], (BLOCK, LANE)) == line
            for n, w in enumerate((lower, upper)):
                term = jnp.where(hit, jnp.broadcast_to(w[l : l + 1, :], (BLOCK, LANE)), none)
                sums[n] = term if sums[n] is None else sums[n] + term
        for n in range(2):
            second = (sums[n] * jnp.asarray(0.0625, BF) + jnp.asarray(128.0, BF)) - jnp.asarray(128.0, BF)
            first = sums[n] - second * jnp.asarray(16.0, BF)
            at = 2 * n * BLOCK
            hold[at : at + BLOCK, q * LANE : (q + 1) * LANE] = first
            hold[at + BLOCK : at + 2 * BLOCK, q * LANE : (q + 1) * LANE] = second
    pooled = jnp.dot(table, hold[...], preferred_element_type=F32).astype(BF)
    return pooled, jnp.dot(down, pooled, preferred_element_type=F32)


def pool0_body(lookups, *refs):
    tables = refs[0:8]
    x0_out, low_out, table_out, factor_out, new_cache = refs[8:13]
    counts, x0, whole_table, factors, sems = refs[13:]
    y = lax.axis_index("y")
    c = lax.axis_index("c")
    low_out[...] = jnp.zeros(low_out.shape, F32)

    def writes(i):
        return [
            pltpu.make_async_copy(source.at[i], out.at[i], sems.at[n, i])
            for n, (source, out) in enumerate(((x0, x0_out), (whole_table, table_out), (factors, factor_out)))
        ]

    def pair(j, _):
        low = None
        for m in range(2):
            i = 2 * j + m
            mine = jnp.concatenate([t[i, :LANE, :] for t in tables[:4]], axis=1)
            theirs = jnp.concatenate([t[i, :LANE, :] for t in tables[4:]], axis=1)
            table = jnp.concatenate([jnp.where(c == 0, mine, theirs), jnp.where(c == 0, theirs, mine)], axis=0)
            whole_table[i] = table
            down = factor(tables, i)
            factors[i] = down
            pooled, part = pool_step(0, i, table, down, lookups, counts.at[m])
            x0[i] = pooled
            low = part if low is None else low + part
            for copy in writes(i):
                copy.start()
        low_out[...] = low_out[...] + low
        return 0

    lax.fori_loop(0, NZ // 2, pair, 0)
    own = whole_table[lax.axis_index("z")]
    for r in range(NY):
        new_cache[(y + r) % NY] = own[:, r * BLOCK : (r + 1) * BLOCK].T
    for i in range(NZ):
        for copy in writes(i):
            copy.wait()


MANY = NX * LANE


def pool0(lookups, tables):
    return kernel(
        pool0_body,
        [pltpu.HBM((NZ, E, MANY), BF), jax.ShapeDtypeStruct((RANK, MANY), F32), pltpu.HBM((NZ, E, SLOTS * BLOCK), BF),
         pltpu.HBM((NZ, RANK, E), BF), bf(SLOTS, BLOCK, E)],
        [VMEM] * 9, [ANY, VMEM, ANY, ANY, VMEM],
        [pltpu.VMEM((2, SLOTS * BLOCK, MANY), BF), pltpu.VMEM((NZ, E, MANY), BF), pltpu.VMEM((NZ, E, SLOTS * BLOCK), BF),
         pltpu.VMEM((NZ, RANK, E), BF), pltpu.SemaphoreType.DMA((3, NZ))],
        flops=1 << 32, limit=24,
    )(*near(lookups, *tables))


def pool1_body(lookups, table_in, factor_in, x0_out, low_out, counts, x0, tables, factors, sems, out_sems):
    low_out[...] = jnp.zeros(low_out.shape, F32)

    def reads(i):
        return [
            pltpu.make_async_copy(source.at[i], hold.at[i], sems.at[n, i])
            for n, (source, hold) in enumerate(((table_in, tables), (factor_in, factors)))
        ]

    def write(i):
        return pltpu.make_async_copy(x0.at[i], x0_out.at[i], out_sems.at[i])

    for i in range(NZ):
        for copy in reads(i):
            copy.start()

    def pair(j, _):
        low = None
        for m in range(2):
            i = 2 * j + m
            for copy in reads(i):
                copy.wait()
            pooled, part = pool_step(1, i, tables[i], factors[i], lookups, counts.at[m])
            x0[i] = pooled
            low = part if low is None else low + part
            write(i).start()
        low_out[...] = low_out[...] + low
        return 0

    lax.fori_loop(0, NZ // 2, pair, 0)
    for i in range(NZ):
        write(i).wait()


def pool1(lookups, table, factors):
    return kernel(
        pool1_body, [pltpu.HBM((NZ, E, MANY), BF), jax.ShapeDtypeStruct((RANK, MANY), F32)],
        [VMEM, ANY, ANY], [ANY, VMEM],
        [pltpu.VMEM((2, SLOTS * BLOCK, MANY), BF), pltpu.VMEM((NZ, E, MANY), BF), pltpu.VMEM((NZ, E, SLOTS * BLOCK), BF),
         pltpu.VMEM((NZ, RANK, E), BF), pltpu.SemaphoreType.DMA((2, NZ)), pltpu.SemaphoreType.DMA((NZ,))],
        flops=1 << 32, limit=24,
    )(*near(lookups), *far(table, factors))


def cross_body(*refs):
    lows = refs[0:4]
    bias = refs[4]
    tops = refs[5:13]
    x0_in = refs[13]
    outs = refs[14:18]
    x0, weights, crossed, hold, sems = refs[18:]
    x = lax.axis_index("x")
    waits = load((x0_in,), (x0,), sems)
    low = (lows[0][...] + lows[1][...] + lows[2][...] + lows[3][...]).astype(BF)
    columns = bias[pl.ds(pl.multiple_of(x * NZ, NZ), NZ), :].T
    for i in range(NZ):
        for copy in waits[i]:
            copy.wait()
        up = jnp.concatenate([t[i, LANE:, :] for t in tops], axis=0)
        gate = lax.dot_general(up, low, (((0,), (0,)), ((), ())), preferred_element_type=F32)
        gate = gate + columns[:, i : i + 1]
        features = x0[i].astype(F32)
        crossed[i * E : (i + 1) * E, :] = (features * gate + features).astype(BF)
        for j in range(8):
            weights[j * LANE : (j + 1) * LANE, i * E : (i + 1) * E] = tops[j][i, :LANE, :]
    part = jnp.dot(weights[...], crossed[...], preferred_element_type=F32).astype(BF)
    for q in range(NX):
        hold[q] = part[:, q * LANE : (q + 1) * LANE]
    for r in range(NX):
        outs[r][...] = hold[(x + r) % NX]


def cross(lows, bias, tops, x0):
    return kernel(
        cross_body, [bf(HID, LANE)] * NX, [VMEM] * 13 + [ANY], [VMEM] * NX,
        [pltpu.VMEM((NZ, E, MANY), BF), pltpu.VMEM((HID, NZ * E), BF), pltpu.VMEM((NZ * E, MANY), BF),
         pltpu.VMEM((NX, HID, LANE), BF), pltpu.SemaphoreType.DMA((1, NZ))],
        flops=1 << 32, limit=32,
    )(*near(*lows, bias, *tops), *far(x0))


def score_body(mlp_bias, mlp_out, out_bias, *refs):
    hs = refs[0:8]
    out, rows = refs[8:]
    y = lax.axis_index("y")
    c = lax.axis_index("c")
    for j in range(8):
        o = ((y + j % 4) % NY) * NC + (c + j // 4) % NC
        rows[j : j + 1, :] = mlp_bias[pl.ds(o, 1), :]
        rows[8 + j : 9 + j, :] = mlp_out[pl.ds(o, 1), :]
    columns = rows[...].T
    for b in range(2):
        total = jnp.zeros((LANE, LANE), F32)
        for j in range(8):
            before = columns[:, j : j + 1]
            for h in hs[4 * b : 4 * b + 4]:
                before = before + h[j * LANE : (j + 1) * LANE, :].astype(F32)
            total = total + jnp.maximum(before, 0.0) * columns[:, 8 + j : 9 + j]
        out[b : b + 1, :] = jnp.sum(total, axis=0, keepdims=True) + out_bias[0]


def score(mlp_bias, mlp_out, out_bias, ha, hb):
    return kernel(
        score_body, jax.ShapeDtypeStruct((2, LANE), F32), [VMEM, VMEM, SMEM] + [VMEM] * 8, VMEM,
        [pltpu.VMEM((16, LANE), F32)],
    )(mlp_bias, mlp_out, out_bias, *near(*ha, *hb))


def shift(v, axis, size, k):
    return lax.ppermute(v, axis, [(i, (i + k) % size) for i in range(size)])


def spread(v, axis, size):
    out = [v]
    for k in range(1, size):
        out.append(shift(v, axis, size, size - k))
    return out


def deal(parts):
    out = [parts[0]]
    for k in range(1, NX):
        out.append(shift(parts[k], "x", NX, k))
    return out


def exchange(v, axis):
    return lax.all_to_all(v, axis, 0, 0, tiled=True)


def swaps(vs):
    return [shift(v, "c", NC, 1) for v in vs]


def tie(v, *others):
    return lax.optimization_barrier((v, *others))[0]


def on_device(
    cache, backing, resident, promote, victim, lookups, route,
    dcn_down, dcn_up, dcn_bias, mlp_in, mlp_bias, mlp_out, out_bias,
):
    cache = cache[0]
    backing = backing[0]
    bias = dcn_bias.reshape(-1, E)
    outgoing = fetch(promote, victim, backing)
    arrived = exchange(outgoing, ("y", "c"))
    wanted = jnp.transpose(lookups[:, :, 0, :], (0, 2, 1))
    sent, factors = route_lookups(wanted, route[:, 0].reshape(2, -1, LANE), dcn_down)
    piece = make_piece(victim, arrived, cache, factors, sent)
    mixed = exchange(piece, "z")
    top = own_weights(dcn_up, mlp_in)
    new_backing = write_back(resident, victim, cache, backing)
    own = spread(mixed[:, :160, :], "y", NY)
    mixed = mixed[:, 160:, :]
    tops = stacked(spread(tie(top, piece), "z", NZ))
    tables = own + swaps(own)
    own = spread(tops, "y", NY)
    tops = own + swaps(own)
    x00, low0, table, factors, new_cache = pool0(mixed, tables)
    lows0 = spread(low0, "x", NX)
    x01, low1 = pool1(tie(mixed, low0), table, factors)
    lows1 = spread(low1, "x", NX)
    h0 = cross(lows0, bias, tops, tie(x00, low1))
    ra = deal(h0)
    h1 = cross(lows1, bias, tops, tie(x01, h0[0]))
    rb = deal(h1)
    scores = score(mlp_bias.reshape(8, LANE), mlp_out.reshape(8, LANE), out_bias, ra, rb)
    return scores[:, None, :], new_cache[None], new_backing[None]


def solution(mesh):
    fine = Mesh(mesh.devices.reshape(NX, NZ, NY, NC), ("x", "z", "y", "c"))
    ca, ow = ("x", "z"), ("y", "c")
    in_specs = (
        P(ca, None, None, None),
        P(ca, ow, None, None),
        P(ca, None),
        P(ca, None),
        P(ca, None),
        P(None, ow, ca, None),
        P(None, ow, None),
        P(ca, None),
        P(None, ca),
        P(),
        P(ca, None),
        P(),
        P(),
        P(),
    )
    out_specs = (
        P(None, ow, ca),
        P(ca, None, None, None),
        P(ca, ow, None, None),
    )
    return jax.shard_map(
        on_device, mesh=fine, in_specs=in_specs, out_specs=out_specs, check_vma=False
    )
```

```python
import jax
import jax.numpy as jnp
from jax import lax
from jax.experimental import pallas as pl
from jax.experimental.pallas import tpu as pltpu
from jax.sharding import Mesh, PartitionSpec as P

BF = jnp.bfloat16
F32 = jnp.float32
NX, NZ, NY, NC = 4, 8, 4, 2
SLOTS, BLOCK, E = 4, 128, 256
HID, RANK = 1024, 128
LANE = 128


SMEM = pl.BlockSpec(memory_space=pltpu.SMEM)
VMEM = pl.BlockSpec(memory_space=pltpu.VMEM)
ANY = pl.BlockSpec(memory_space=pl.ANY)


def near(*vs):
    return [pltpu.with_memory_space_constraint(v, pltpu.VMEM) for v in vs]


def far(*vs):
    return [pltpu.with_memory_space_constraint(v, pltpu.HBM) for v in vs]


def kernel(body, out_shape, in_specs, out_specs, scratch=(), flops=0, limit=16):
    return pl.pallas_call(
        body,
        out_shape=out_shape,
        in_specs=in_specs,
        out_specs=out_specs,
        scratch_shapes=list(scratch),
        compiler_params=pltpu.CompilerParams(vmem_limit_bytes=limit * 1024 * 1024),
        cost_estimate=pl.CostEstimate(flops=flops, bytes_accessed=0, transcendentals=0),
    )


def bf(*shape):
    return jax.ShapeDtypeStruct(shape, BF)


def fetch_body(promote_in, victim_in, backing, out, promote, victim, blocks, sems):
    count = backing.shape[0]
    base = (lax.axis_index("y") * NC + lax.axis_index("c")) * count
    small = [
        pltpu.make_async_copy(promote_in, promote, sems.at[2]),
        pltpu.make_async_copy(victim_in, victim, sems.at[3]),
    ]
    for copy in small:
        copy.start()
    out[...] = jnp.zeros(out.shape, BF)
    for copy in small:
        copy.wait()
    copies = []
    for k in range(2):
        at = jnp.clip(promote[0, k] - base, 0, count - 1)
        copies.append(pltpu.make_async_copy(backing.at[at], blocks.at[k], sems.at[k]))
    for copy in copies:
        copy.start()
    for copy in copies:
        copy.wait()
    for k in range(2):
        local = promote[0, k] - base

        @pl.when((local >= 0) & (local < count))
        def _():
            s = victim[0, k]
            out[2 * s] = blocks[k, :, :LANE]
            out[2 * s + 1] = blocks[k, :, LANE:]


def fetch(promote, victim, backing):
    return kernel(
        fetch_body, bf(NY * NC, BLOCK, LANE), [ANY] * 3, VMEM,
        [pltpu.SMEM((1, 2), jnp.int32), pltpu.SMEM((1, 2), jnp.int32),
         pltpu.VMEM((2, BLOCK, E), BF), pltpu.SemaphoreType.DMA((4,))],
    )(*far(promote, victim, backing))


def piece_body(victim, arrived, cache, factors, sent, out):
    s = lax.axis_index("y")
    c = lax.axis_index("c")
    total = arrived[0]
    for i in range(1, NY * NC):
        total = total + arrived[i]
    block = cache[s]
    kept = jnp.where(c == 0, block[:, :LANE], block[:, LANE:])
    evicted = (victim[0, 0] == s) | (victim[0, 1] == s)
    piece = jnp.where(evicted, total, kept).T
    for i in range(NZ):
        out[i, :LANE, :] = piece
        out[i, LANE:160, :] = factors[...]
        out[i, 160:, :] = sent[i]


def make_piece(victim, arrived, cache, factors, sent):
    return kernel(
        piece_body, bf(NZ, 224, BLOCK), [SMEM] + [VMEM] * 4, VMEM
    )(victim, *near(arrived, cache, factors, sent))


def back_body(resident, victim, cache, backing, out):
    base = (lax.axis_index("y") * NC + lax.axis_index("c")) * backing.shape[0]
    out[...] = backing[...]
    for k in range(2):
        v = victim[0, k]
        local = resident[0, v] - base

        @pl.when((local >= 0) & (local < backing.shape[0]))
        def _():
            out[local] = cache[v]


def write_back(resident, victim, cache, backing):
    return kernel(
        back_body, jax.ShapeDtypeStruct(backing.shape, BF), [SMEM, SMEM, VMEM, VMEM], VMEM
    )(resident, victim, cache, backing)


def route_body(lookups_in, route_in, down_in, out, factors, lookups, route, down, scratch, sems):
    copies = [
        pltpu.make_async_copy(source, hold, sems.at[n])
        for n, (source, hold) in enumerate(((down_in, down), (route_in, route), (lookups_in, lookups)))
    ]
    for copy in copies:
        copy.start()
    copies[0].wait()
    o = lax.axis_index("y") * NC + lax.axis_index("c")
    rows = RANK // (NY * NC)
    scratch[...] = down[...].T
    piece = scratch[pl.ds(pl.multiple_of(o * rows, rows), rows), :]
    factors[0:16, :] = piece[:, :LANE]
    factors[16:32, :] = piece[:, LANE:]
    copies[1].wait()
    copies[2].wait()
    batches, bag, count = lookups.shape
    tiles = count // LANE

    def one(z, _):
        for q in range(NX):
            parts = []
            for b in range(batches):
                row = jnp.broadcast_to(route[b, pl.ds(q * NZ + z, 1), :], (bag, LANE))
                lane = row & (LANE - 1)
                tile = row >> 7
                got = jnp.zeros((bag, LANE), jnp.int32)
                for v in range(tiles):
                    cand = jnp.take_along_axis(
                        lookups[b, :, v * LANE : (v + 1) * LANE], lane, axis=1, mode="promise_in_bounds"
                    )
                    got = jnp.where(tile == v, cand, got)
                parts.append(got)
            both = (jnp.concatenate(parts, axis=0) - 256).astype(F32).astype(BF)
            out[z, q * 16 : q * 16 + 16, :] = both
        return 0

    lax.fori_loop(0, NZ, one, 0)


def route_lookups(lookups, route, down):
    return kernel(
        route_body, [bf(NZ, 64, LANE), bf(32, LANE)], [ANY] * 3, [VMEM] * 2,
        [pltpu.VMEM(lookups.shape, jnp.int32), pltpu.VMEM(route.shape, jnp.int32), pltpu.VMEM(down.shape, BF),
         pltpu.VMEM((RANK, E), BF), pltpu.SemaphoreType.DMA((3,))],
        flops=1 << 22,
    )(*far(lookups, route, down))


def own_body(up, mlp, out):
    o = lax.axis_index("y") * NC + lax.axis_index("c")
    rows = RANK // (NY * NC)
    out[:LANE, :] = mlp[:, pl.ds(pl.multiple_of(o * LANE, LANE), LANE)].T
    out[LANE:, :] = up[pl.ds(pl.multiple_of(o * rows, rows), rows), :]


def own_weights(up, mlp):
    return kernel(own_body, bf(LANE + 16, E), [VMEM] * 2, VMEM)(up, mlp)


def stack_body(*refs):
    out = refs[-1]
    z = lax.axis_index("z")
    for k in range(NZ):
        out[(z + k) % NZ] = refs[k][...]


def stacked(parts):
    return kernel(stack_body, bf(NZ, LANE + 16, E), [VMEM] * NZ, VMEM)(*near(*parts))


def factor(tables, i):
    rows = [jnp.concatenate([t[i, LANE : LANE + 16, :], t[i, LANE + 16 :, :]], axis=1) for t in tables]
    return jnp.concatenate(rows, axis=0)


def load(sources, holds, sems):
    waits = []
    for i in range(NZ):
        step = []
        for n, (source, hold) in enumerate(zip(sources, holds)):
            copy = pltpu.make_async_copy(source.at[i], hold.at[i], sems.at[n, i])
            copy.start()
            step.append(copy)
        waits.append(step)
    return waits


def pool_step(batch, i, table, down, lookups, hold):
    y = lax.axis_index("y")
    line = lax.broadcasted_iota(jnp.int32, (BLOCK, LANE), 0).astype(F32).astype(BF)
    none = jnp.zeros((), BF)
    for q in range(NX):
        wanted = lookups[i, q * 16 + batch * 8 : q * 16 + batch * 8 + 8, :]
        wanted = wanted.astype(F32).astype(jnp.int32) + 256
        slot = ((wanted >> 7) + (NY - y)) & 3
        weight = jnp.where((slot & 1) == 1, 16.0, 1.0)
        row = (wanted & (BLOCK - 1)).astype(F32).astype(BF)
        lower = jnp.where(slot < 2, weight, 0.0).astype(BF)
        upper = jnp.where(slot < 2, 0.0, weight).astype(BF)
        sums = [None, None]
        for l in range(8):
            hit = jnp.broadcast_to(row[l : l + 1, :], (BLOCK, LANE)) == line
            for n, w in enumerate((lower, upper)):
                term = jnp.where(hit, jnp.broadcast_to(w[l : l + 1, :], (BLOCK, LANE)), none)
                sums[n] = term if sums[n] is None else sums[n] + term
        for n in range(2):
            second = (sums[n] * jnp.asarray(0.0625, BF) + jnp.asarray(128.0, BF)) - jnp.asarray(128.0, BF)
            first = sums[n] - second * jnp.asarray(16.0, BF)
            at = 2 * n * BLOCK
            hold[at : at + BLOCK, q * LANE : (q + 1) * LANE] = first
            hold[at + BLOCK : at + 2 * BLOCK, q * LANE : (q + 1) * LANE] = second
    pooled = jnp.dot(table, hold[...], preferred_element_type=F32).astype(BF)
    return pooled, jnp.dot(down, pooled, preferred_element_type=F32)


def pool0_body(lookups, *refs):
    tables = refs[0:8]
    x0_out, low_out, table_out, factor_out, new_cache = refs[8:13]
    counts, x0, whole_table, factors, sems = refs[13:]
    y = lax.axis_index("y")
    c = lax.axis_index("c")
    low_out[...] = jnp.zeros(low_out.shape, F32)

    def writes(i):
        return [
            pltpu.make_async_copy(source.at[i], out.at[i], sems.at[n, i])
            for n, (source, out) in enumerate(((x0, x0_out), (whole_table, table_out), (factors, factor_out)))
        ]

    def pair(j, _):
        low = None
        for m in range(2):
            i = 2 * j + m
            mine = jnp.concatenate([t[i, :LANE, :] for t in tables[:4]], axis=1)
            theirs = jnp.concatenate([t[i, :LANE, :] for t in tables[4:]], axis=1)
            table = jnp.concatenate([jnp.where(c == 0, mine, theirs), jnp.where(c == 0, theirs, mine)], axis=0)
            whole_table[i] = table
            down = factor(tables, i)
            factors[i] = down
            pooled, part = pool_step(0, i, table, down, lookups, counts.at[m])
            x0[i] = pooled
            low = part if low is None else low + part
            for copy in writes(i):
                copy.start()
        low_out[...] = low_out[...] + low
        return 0

    lax.fori_loop(0, NZ // 2, pair, 0)
    own = whole_table[lax.axis_index("z")]
    for r in range(NY):
        new_cache[(y + r) % NY] = own[:, r * BLOCK : (r + 1) * BLOCK].T
    for i in range(NZ):
        for copy in writes(i):
            copy.wait()


MANY = NX * LANE


def pool0(lookups, tables):
    return kernel(
        pool0_body,
        [pltpu.HBM((NZ, E, MANY), BF), jax.ShapeDtypeStruct((RANK, MANY), F32), pltpu.HBM((NZ, E, SLOTS * BLOCK), BF),
         pltpu.HBM((NZ, RANK, E), BF), bf(SLOTS, BLOCK, E)],
        [VMEM] * 9, [ANY, VMEM, ANY, ANY, VMEM],
        [pltpu.VMEM((2, SLOTS * BLOCK, MANY), BF), pltpu.VMEM((NZ, E, MANY), BF), pltpu.VMEM((NZ, E, SLOTS * BLOCK), BF),
         pltpu.VMEM((NZ, RANK, E), BF), pltpu.SemaphoreType.DMA((3, NZ))],
        flops=1 << 32, limit=24,
    )(*near(lookups, *tables))


def pool1_body(lookups, table_in, factor_in, x0_out, low_out, counts, x0, tables, factors, sems, out_sems):
    low_out[...] = jnp.zeros(low_out.shape, F32)

    def reads(i):
        return [
            pltpu.make_async_copy(source.at[i], hold.at[i], sems.at[n, i])
            for n, (source, hold) in enumerate(((table_in, tables), (factor_in, factors)))
        ]

    def write(i):
        return pltpu.make_async_copy(x0.at[i], x0_out.at[i], out_sems.at[i])

    for i in range(NZ):
        for copy in reads(i):
            copy.start()

    def pair(j, _):
        low = None
        for m in range(2):
            i = 2 * j + m
            for copy in reads(i):
                copy.wait()
            pooled, part = pool_step(1, i, tables[i], factors[i], lookups, counts.at[m])
            x0[i] = pooled
            low = part if low is None else low + part
            write(i).start()
        low_out[...] = low_out[...] + low
        return 0

    lax.fori_loop(0, NZ // 2, pair, 0)
    for i in range(NZ):
        write(i).wait()


def pool1(lookups, table, factors):
    return kernel(
        pool1_body, [pltpu.HBM((NZ, E, MANY), BF), jax.ShapeDtypeStruct((RANK, MANY), F32)],
        [VMEM, ANY, ANY], [ANY, VMEM],
        [pltpu.VMEM((2, SLOTS * BLOCK, MANY), BF), pltpu.VMEM((NZ, E, MANY), BF), pltpu.VMEM((NZ, E, SLOTS * BLOCK), BF),
         pltpu.VMEM((NZ, RANK, E), BF), pltpu.SemaphoreType.DMA((2, NZ)), pltpu.SemaphoreType.DMA((NZ,))],
        flops=1 << 32, limit=24,
    )(*near(lookups), *far(table, factors))


def cross_body(*refs):
    lows = refs[0:4]
    bias = refs[4]
    tops = refs[5:15]
    x0_in = refs[15]
    outs = refs[16:20]
    x0, weights, crossed, hold, sems = refs[20:]
    x = lax.axis_index("x")
    waits = load((x0_in,), (x0,), sems)
    low = (lows[0][...] + lows[1][...] + lows[2][...] + lows[3][...]).astype(BF)
    columns = bias[pl.ds(pl.multiple_of(x * NZ, NZ), NZ), :].T
    for i in range(NZ):
        for copy in waits[i]:
            copy.wait()
        at = i % (NZ // 2)
        pieces = []
        for side in (tops[:5], tops[5:]):
            across = side[3][at] if i < NZ // 2 else side[4][at]
            pieces += [side[0][i], side[1][i], across, side[2][i]]
        up = jnp.concatenate([t[LANE:, :] for t in pieces], axis=0)
        gate = lax.dot_general(up, low, (((0,), (0,)), ((), ())), preferred_element_type=F32)
        gate = gate + columns[:, i : i + 1]
        features = x0[i].astype(F32)
        crossed[i * E : (i + 1) * E, :] = (features * gate + features).astype(BF)
        for j in range(8):
            weights[j * LANE : (j + 1) * LANE, i * E : (i + 1) * E] = pieces[j][:LANE, :]
    part = jnp.dot(weights[...], crossed[...], preferred_element_type=F32).astype(BF)
    for q in range(NX):
        hold[q] = part[:, q * LANE : (q + 1) * LANE]
    for r in range(NX):
        outs[r][...] = hold[(x + r) % NX]


def cross(lows, bias, tops, x0):
    return kernel(
        cross_body, [bf(HID, LANE)] * NX, [VMEM] * 15 + [ANY], [VMEM] * NX,
        [pltpu.VMEM((NZ, E, MANY), BF), pltpu.VMEM((HID, NZ * E), BF), pltpu.VMEM((NZ * E, MANY), BF),
         pltpu.VMEM((NX, HID, LANE), BF), pltpu.SemaphoreType.DMA((1, NZ))],
        flops=1 << 32, limit=32,
    )(*near(*lows, bias, *tops), *far(x0))


def score_body(mlp_bias, mlp_out, out_bias, *refs):
    hs = refs[0:8]
    out, rows = refs[8:]
    y = lax.axis_index("y")
    c = lax.axis_index("c")
    for j in range(8):
        o = ((y + j % 4) % NY) * NC + (c + j // 4) % NC
        rows[j : j + 1, :] = mlp_bias[pl.ds(o, 1), :]
        rows[8 + j : 9 + j, :] = mlp_out[pl.ds(o, 1), :]
    columns = rows[...].T
    for b in range(2):
        total = jnp.zeros((LANE, LANE), F32)
        for j in range(8):
            before = columns[:, j : j + 1]
            for h in hs[4 * b : 4 * b + 4]:
                before = before + h[j * LANE : (j + 1) * LANE, :].astype(F32)
            total = total + jnp.maximum(before, 0.0) * columns[:, 8 + j : 9 + j]
        out[b : b + 1, :] = jnp.sum(total, axis=0, keepdims=True) + out_bias[0]


def score(mlp_bias, mlp_out, out_bias, ha, hb):
    return kernel(
        score_body, jax.ShapeDtypeStruct((2, LANE), F32), [VMEM, VMEM, SMEM] + [VMEM] * 8, VMEM,
        [pltpu.VMEM((16, LANE), F32)],
    )(mlp_bias, mlp_out, out_bias, *near(*ha, *hb))


def shift(v, axis, size, k):
    return lax.ppermute(v, axis, [(i, (i + k) % size) for i in range(size)])


def spread(v, axis, size):
    out = [v]
    for k in range(1, size):
        out.append(shift(v, axis, size, size - k))
    return out


def around(v):
    half = NZ // 2
    after = shift(v, "y", NY, NY - 1)
    before = shift(v, "y", NY, 1)
    first = shift(after[:half], "y", NY, NY - 1)
    second = shift(before[half:], "y", NY, 1)
    return [v, after, before, first, second]


def deal(parts):
    out = [parts[0]]
    for k in range(1, NX):
        out.append(shift(parts[k], "x", NX, k))
    return out


def exchange(v, axis):
    return lax.all_to_all(v, axis, 0, 0, tiled=True)


def swaps(vs):
    return [shift(v, "c", NC, 1) for v in vs]


def tie(v, *others):
    return lax.optimization_barrier((v, *others))[0]


def on_device(
    cache, backing, resident, promote, victim, lookups, route,
    dcn_down, dcn_up, dcn_bias, mlp_in, mlp_bias, mlp_out, out_bias,
):
    cache = cache[0]
    backing = backing[0]
    bias = dcn_bias.reshape(-1, E)
    outgoing = fetch(promote, victim, backing)
    arrived = exchange(outgoing, ("y", "c"))
    wanted = jnp.transpose(lookups[:, :, 0, :], (0, 2, 1))
    sent, factors = route_lookups(wanted, route[:, 0].reshape(2, -1, LANE), dcn_down)
    piece = make_piece(victim, arrived, cache, factors, sent)
    mixed = exchange(piece, "z")
    top = own_weights(dcn_up, mlp_in)
    own = spread(mixed[:, :160, :], "y", NY)
    mixed = mixed[:, 160:, :]
    tops = stacked(spread(tie(top, piece), "z", NZ))
    tables = own + swaps(own)
    own = around(tops)
    tops = own + swaps(own)
    x00, low0, table, factors, new_cache = pool0(mixed, tables)
    lows0 = spread(low0, "x", NX)
    x01, low1 = pool1(tie(mixed, low0, bias), table, factors)
    lows1 = spread(low1, "x", NX)
    h0 = cross(lows0, bias, tops, tie(x00, low1))
    ra = deal(h0)
    h1 = cross(lows1, bias, tops, tie(x01, h0[0]))
    rb = deal(h1)
    new_backing = write_back(resident, victim, cache, tie(backing, h1[0]))
    scores = score(mlp_bias.reshape(8, LANE), mlp_out.reshape(8, LANE), out_bias, ra, rb)
    return scores[:, None, :], new_cache[None], new_backing[None]


def solution(mesh):
    fine = Mesh(mesh.devices.reshape(NX, NZ, NY, NC), ("x", "z", "y", "c"))
    ca, ow = ("x", "z"), ("y", "c")
    in_specs = (
        P(ca, None, None, None),
        P(ca, ow, None, None),
        P(ca, None),
        P(ca, None),
        P(ca, None),
        P(None, ow, ca, None),
        P(None, ow, None),
        P(ca, None),
        P(None, ca),
        P(),
        P(ca, None),
        P(),
        P(),
        P(),
    )
    out_specs = (
        P(None, ow, ca),
        P(ca, None, None, None),
        P(ca, ow, None, None),
    )
    return jax.shard_map(
        on_device, mesh=fine, in_specs=in_specs, out_specs=out_specs, check_vma=False
    )
```

```python
import jax
import jax.numpy as jnp
from jax import lax
from jax.experimental import pallas as pl
from jax.experimental.pallas import tpu as pltpu
from jax.sharding import Mesh, PartitionSpec as P

BF = jnp.bfloat16
F32 = jnp.float32
NX, NZ, NY, NC = 4, 8, 4, 2
SLOTS, BLOCK, E = 4, 128, 256
HID, RANK = 1024, 128
LANE = 128


SMEM = pl.BlockSpec(memory_space=pltpu.SMEM)
VMEM = pl.BlockSpec(memory_space=pltpu.VMEM)
ANY = pl.BlockSpec(memory_space=pl.ANY)


def near(*vs):
    return [pltpu.with_memory_space_constraint(v, pltpu.VMEM) for v in vs]


def far(*vs):
    return [pltpu.with_memory_space_constraint(v, pltpu.HBM) for v in vs]


def kernel(body, out_shape, in_specs, out_specs, scratch=(), flops=0, limit=16):
    return pl.pallas_call(
        body,
        out_shape=out_shape,
        in_specs=in_specs,
        out_specs=out_specs,
        scratch_shapes=list(scratch),
        compiler_params=pltpu.CompilerParams(vmem_limit_bytes=limit * 1024 * 1024),
        cost_estimate=pl.CostEstimate(flops=flops, bytes_accessed=0, transcendentals=0),
    )


def bf(*shape):
    return jax.ShapeDtypeStruct(shape, BF)


def fetch_body(promote_in, victim_in, backing, out, promote, victim, blocks, sems):
    count = backing.shape[0]
    base = (lax.axis_index("y") * NC + lax.axis_index("c")) * count
    small = [
        pltpu.make_async_copy(promote_in, promote, sems.at[2]),
        pltpu.make_async_copy(victim_in, victim, sems.at[3]),
    ]
    for copy in small:
        copy.start()
    out[...] = jnp.zeros(out.shape, BF)
    for copy in small:
        copy.wait()
    copies = []
    for k in range(2):
        at = jnp.clip(promote[0, k] - base, 0, count - 1)
        copies.append(pltpu.make_async_copy(backing.at[at], blocks.at[k], sems.at[k]))
    for copy in copies:
        copy.start()
    for copy in copies:
        copy.wait()
    for k in range(2):
        local = promote[0, k] - base

        @pl.when((local >= 0) & (local < count))
        def _():
            s = victim[0, k]
            out[2 * s] = blocks[k, :, :LANE]
            out[2 * s + 1] = blocks[k, :, LANE:]


def fetch(promote, victim, backing):
    return kernel(
        fetch_body, bf(NY * NC, BLOCK, LANE), [ANY] * 3, VMEM,
        [pltpu.SMEM((1, 2), jnp.int32), pltpu.SMEM((1, 2), jnp.int32),
         pltpu.VMEM((2, BLOCK, E), BF), pltpu.SemaphoreType.DMA((4,))],
    )(*far(promote, victim, backing))


def piece_body(victim_in, cache_in, arrived, factors, sent, out, victim, cache, sems):
    s = lax.axis_index("y")
    c = lax.axis_index("c")
    copies = [
        pltpu.make_async_copy(victim_in, victim, sems.at[0]),
        pltpu.make_async_copy(cache_in.at[s], cache, sems.at[1]),
    ]
    for copy in copies:
        copy.start()
    total = arrived[0]
    for i in range(1, NY * NC):
        total = total + arrived[i]
    for copy in copies:
        copy.wait()
    block = cache[...]
    kept = jnp.where(c == 0, block[:, :LANE], block[:, LANE:])
    evicted = (victim[0, 0] == s) | (victim[0, 1] == s)
    piece = jnp.where(evicted, total, kept).T
    for i in range(NZ):
        out[i, :LANE, :] = piece
        out[i, LANE:160, :] = factors[...]
        out[i, 160:, :] = sent[i]


def make_piece(victim, arrived, cache, factors, sent):
    return kernel(
        piece_body, bf(NZ, 224, BLOCK), [ANY] * 2 + [VMEM] * 3, VMEM,
        [pltpu.SMEM((1, 2), jnp.int32), pltpu.VMEM((BLOCK, E), BF), pltpu.SemaphoreType.DMA((2,))],
    )(*far(victim, cache), *near(arrived, factors, sent))


def back_body(resident, victim, cache, backing, out):
    base = (lax.axis_index("y") * NC + lax.axis_index("c")) * backing.shape[0]
    out[...] = backing[...]
    for k in range(2):
        v = victim[0, k]
        local = resident[0, v] - base

        @pl.when((local >= 0) & (local < backing.shape[0]))
        def _():
            out[local] = cache[v]


def write_back(resident, victim, cache, backing):
    return kernel(
        back_body, jax.ShapeDtypeStruct(backing.shape, BF), [SMEM, SMEM, VMEM, VMEM], VMEM
    )(resident, victim, cache, backing)


def route_body(lookups_in, route_in, down_in, out, factors, lookups, route, down, scratch, sems):
    copies = [
        pltpu.make_async_copy(source, hold, sems.at[n])
        for n, (source, hold) in enumerate(((down_in, down), (route_in, route), (lookups_in, lookups)))
    ]
    for copy in copies:
        copy.start()
    copies[0].wait()
    o = lax.axis_index("y") * NC + lax.axis_index("c")
    rows = RANK // (NY * NC)
    scratch[...] = down[...].T
    piece = scratch[pl.ds(pl.multiple_of(o * rows, rows), rows), :]
    factors[0:16, :] = piece[:, :LANE]
    factors[16:32, :] = piece[:, LANE:]
    copies[1].wait()
    copies[2].wait()
    batches, bag, count = lookups.shape
    tiles = count // LANE

    def one(z, _):
        for q in range(NX):
            parts = []
            for b in range(batches):
                row = jnp.broadcast_to(route[b, pl.ds(q * NZ + z, 1), :], (bag, LANE))
                lane = row & (LANE - 1)
                tile = row >> 7
                got = jnp.zeros((bag, LANE), jnp.int32)
                for v in range(tiles):
                    cand = jnp.take_along_axis(
                        lookups[b, :, v * LANE : (v + 1) * LANE], lane, axis=1, mode="promise_in_bounds"
                    )
                    got = jnp.where(tile == v, cand, got)
                parts.append(got)
            both = (jnp.concatenate(parts, axis=0) - 256).astype(F32).astype(BF)
            out[z, q * 16 : q * 16 + 16, :] = both
        return 0

    lax.fori_loop(0, NZ, one, 0)


def route_lookups(lookups, route, down):
    return kernel(
        route_body, [bf(NZ, 64, LANE), bf(32, LANE)], [ANY] * 3, [VMEM] * 2,
        [pltpu.VMEM(lookups.shape, jnp.int32), pltpu.VMEM(route.shape, jnp.int32), pltpu.VMEM(down.shape, BF),
         pltpu.VMEM((RANK, E), BF), pltpu.SemaphoreType.DMA((3,))],
        flops=1 << 22,
    )(*far(lookups, route, down))


def own_body(up, mlp, out):
    o = lax.axis_index("y") * NC + lax.axis_index("c")
    rows = RANK // (NY * NC)
    out[:LANE, :] = mlp[:, pl.ds(pl.multiple_of(o * LANE, LANE), LANE)].T
    out[LANE:, :] = up[pl.ds(pl.multiple_of(o * rows, rows), rows), :]


def own_weights(up, mlp):
    return kernel(own_body, bf(LANE + 16, E), [VMEM] * 2, VMEM)(up, mlp)


def stack_body(*refs):
    out = refs[-1]
    z = lax.axis_index("z")
    for k in range(NZ):
        out[(z + k) % NZ] = refs[k][...]


def stacked(parts):
    return kernel(stack_body, bf(NZ, LANE + 16, E), [VMEM] * NZ, VMEM)(*near(*parts))


def factor(tables, i):
    rows = [jnp.concatenate([t[i, LANE : LANE + 16, :], t[i, LANE + 16 :, :]], axis=1) for t in tables]
    return jnp.concatenate(rows, axis=0)


def load(sources, holds, sems):
    waits = []
    for i in range(NZ):
        step = []
        for n, (source, hold) in enumerate(zip(sources, holds)):
            copy = pltpu.make_async_copy(source.at[i], hold.at[i], sems.at[n, i])
            copy.start()
            step.append(copy)
        waits.append(step)
    return waits


def pool_step(batch, i, table, down, lookups, hold):
    y = lax.axis_index("y")
    line = lax.broadcasted_iota(jnp.int32, (BLOCK, LANE), 0).astype(F32).astype(BF)
    none = jnp.zeros((), BF)
    for q in range(NX):
        wanted = lookups[i, q * 16 + batch * 8 : q * 16 + batch * 8 + 8, :]
        wanted = wanted.astype(F32).astype(jnp.int32) + 256
        slot = ((wanted >> 7) + (NY - y)) & 3
        weight = jnp.where((slot & 1) == 1, 16.0, 1.0)
        row = (wanted & (BLOCK - 1)).astype(F32).astype(BF)
        lower = jnp.where(slot < 2, weight, 0.0).astype(BF)
        upper = jnp.where(slot < 2, 0.0, weight).astype(BF)
        sums = [None, None]
        for l in range(8):
            hit = jnp.broadcast_to(row[l : l + 1, :], (BLOCK, LANE)) == line
            for n, w in enumerate((lower, upper)):
                term = jnp.where(hit, jnp.broadcast_to(w[l : l + 1, :], (BLOCK, LANE)), none)
                sums[n] = term if sums[n] is None else sums[n] + term
        for n in range(2):
            second = (sums[n] * jnp.asarray(0.0625, BF) + jnp.asarray(128.0, BF)) - jnp.asarray(128.0, BF)
            first = sums[n] - second * jnp.asarray(16.0, BF)
            at = 2 * n * BLOCK
            hold[at : at + BLOCK, q * LANE : (q + 1) * LANE] = first
            hold[at + BLOCK : at + 2 * BLOCK, q * LANE : (q + 1) * LANE] = second
    pooled = jnp.dot(table, hold[...], preferred_element_type=F32).astype(BF)
    return pooled, jnp.dot(down, pooled, preferred_element_type=F32)


def pool0_body(lookups, *refs):
    tables = refs[0:8]
    x0_out, low_out, table_out, factor_out, new_cache = refs[8:13]
    counts, x0, whole_table, factors, sems = refs[13:]
    y = lax.axis_index("y")
    c = lax.axis_index("c")
    low_out[...] = jnp.zeros(low_out.shape, F32)

    def writes(i):
        return [
            pltpu.make_async_copy(source.at[i], out.at[i], sems.at[n, i])
            for n, (source, out) in enumerate(((x0, x0_out), (whole_table, table_out), (factors, factor_out)))
        ]

    def pair(j, _):
        low = None
        for m in range(2):
            i = 2 * j + m
            mine = jnp.concatenate([t[i, :LANE, :] for t in tables[:4]], axis=1)
            theirs = jnp.concatenate([t[i, :LANE, :] for t in tables[4:]], axis=1)
            table = jnp.concatenate([jnp.where(c == 0, mine, theirs), jnp.where(c == 0, theirs, mine)], axis=0)
            whole_table[i] = table
            down = factor(tables, i)
            factors[i] = down
            pooled, part = pool_step(0, i, table, down, lookups, counts.at[m])
            x0[i] = pooled
            low = part if low is None else low + part
            for copy in writes(i):
                copy.start()
        low_out[...] = low_out[...] + low
        return 0

    lax.fori_loop(0, NZ // 2, pair, 0)
    own = whole_table[lax.axis_index("z")]
    for r in range(NY):
        new_cache[(y + r) % NY] = own[:, r * BLOCK : (r + 1) * BLOCK].T
    for i in range(NZ):
        for copy in writes(i):
            copy.wait()


MANY = NX * LANE


def pool0(lookups, tables):
    return kernel(
        pool0_body,
        [pltpu.HBM((NZ, E, MANY), BF), jax.ShapeDtypeStruct((RANK, MANY), F32), pltpu.HBM((NZ, E, SLOTS * BLOCK), BF),
         pltpu.HBM((NZ, RANK, E), BF), bf(SLOTS, BLOCK, E)],
        [VMEM] * 9, [ANY, VMEM, ANY, ANY, VMEM],
        [pltpu.VMEM((2, SLOTS * BLOCK, MANY), BF), pltpu.VMEM((NZ, E, MANY), BF), pltpu.VMEM((NZ, E, SLOTS * BLOCK), BF),
         pltpu.VMEM((NZ, RANK, E), BF), pltpu.SemaphoreType.DMA((3, NZ))],
        flops=1 << 32, limit=24,
    )(*near(lookups, *tables))


def pool1_body(lookups, table_in, factor_in, x0_out, low_out, counts, x0, tables, factors, sems, out_sems):
    low_out[...] = jnp.zeros(low_out.shape, F32)

    def reads(i):
        return [
            pltpu.make_async_copy(source.at[i], hold.at[i], sems.at[n, i])
            for n, (source, hold) in enumerate(((table_in, tables), (factor_in, factors)))
        ]

    def write(i):
        return pltpu.make_async_copy(x0.at[i], x0_out.at[i], out_sems.at[i])

    for i in range(NZ):
        for copy in reads(i):
            copy.start()

    def pair(j, _):
        low = None
        for m in range(2):
            i = 2 * j + m
            for copy in reads(i):
                copy.wait()
            pooled, part = pool_step(1, i, tables[i], factors[i], lookups, counts.at[m])
            x0[i] = pooled
            low = part if low is None else low + part
            write(i).start()
        low_out[...] = low_out[...] + low
        return 0

    lax.fori_loop(0, NZ // 2, pair, 0)
    for i in range(NZ):
        write(i).wait()


def pool1(lookups, table, factors):
    return kernel(
        pool1_body, [pltpu.HBM((NZ, E, MANY), BF), jax.ShapeDtypeStruct((RANK, MANY), F32)],
        [VMEM, ANY, ANY], [ANY, VMEM],
        [pltpu.VMEM((2, SLOTS * BLOCK, MANY), BF), pltpu.VMEM((NZ, E, MANY), BF), pltpu.VMEM((NZ, E, SLOTS * BLOCK), BF),
         pltpu.VMEM((NZ, RANK, E), BF), pltpu.SemaphoreType.DMA((2, NZ)), pltpu.SemaphoreType.DMA((NZ,))],
        flops=1 << 32, limit=24,
    )(*near(lookups), *far(table, factors))


def cross_body(*refs):
    lows = refs[0:4]
    bias = refs[4]
    tops = refs[5:15]
    x0_in = refs[15]
    outs = refs[16:20]
    x0, weights, crossed, hold, sems = refs[20:]
    x = lax.axis_index("x")
    waits = load((x0_in,), (x0,), sems)
    low = (lows[0][...] + lows[1][...] + lows[2][...] + lows[3][...]).astype(BF)
    columns = bias[pl.ds(pl.multiple_of(x * NZ, NZ), NZ), :].T
    for i in range(NZ):
        for copy in waits[i]:
            copy.wait()
        at = i % (NZ // 2)
        pieces = []
        for side in (tops[:5], tops[5:]):
            across = side[3][at] if i < NZ // 2 else side[4][at]
            pieces += [side[0][i], side[1][i], across, side[2][i]]
        up = jnp.concatenate([t[LANE:, :] for t in pieces], axis=0)
        gate = lax.dot_general(up, low, (((0,), (0,)), ((), ())), preferred_element_type=F32)
        gate = gate + columns[:, i : i + 1]
        features = x0[i].astype(F32)
        crossed[i * E : (i + 1) * E, :] = (features * gate + features).astype(BF)
        for j in range(8):
            weights[j * LANE : (j + 1) * LANE, i * E : (i + 1) * E] = pieces[j][:LANE, :]
    part = jnp.dot(weights[...], crossed[...], preferred_element_type=F32).astype(BF)
    for q in range(NX):
        hold[q] = part[:, q * LANE : (q + 1) * LANE]
    for r in range(NX):
        outs[r][...] = hold[(x + r) % NX]


def cross(lows, bias, tops, x0):
    return kernel(
        cross_body, [bf(HID, LANE)] * NX, [VMEM] * 15 + [ANY], [VMEM] * NX,
        [pltpu.VMEM((NZ, E, MANY), BF), pltpu.VMEM((HID, NZ * E), BF), pltpu.VMEM((NZ * E, MANY), BF),
         pltpu.VMEM((NX, HID, LANE), BF), pltpu.SemaphoreType.DMA((1, NZ))],
        flops=1 << 32, limit=32,
    )(*near(*lows, bias, *tops), *far(x0))


def score_body(mlp_bias, mlp_out, out_bias, *refs):
    hs = refs[0:8]
    out, rows = refs[8:]
    y = lax.axis_index("y")
    c = lax.axis_index("c")
    for j in range(8):
        o = ((y + j % 4) % NY) * NC + (c + j // 4) % NC
        rows[j : j + 1, :] = mlp_bias[pl.ds(o, 1), :]
        rows[8 + j : 9 + j, :] = mlp_out[pl.ds(o, 1), :]
    columns = rows[...].T
    for b in range(2):
        total = jnp.zeros((LANE, LANE), F32)
        for j in range(8):
            before = columns[:, j : j + 1]
            for h in hs[4 * b : 4 * b + 4]:
                before = before + h[j * LANE : (j + 1) * LANE, :].astype(F32)
            total = total + jnp.maximum(before, 0.0) * columns[:, 8 + j : 9 + j]
        out[b : b + 1, :] = jnp.sum(total, axis=0, keepdims=True) + out_bias[0]


def score(mlp_bias, mlp_out, out_bias, ha, hb):
    return kernel(
        score_body, jax.ShapeDtypeStruct((2, LANE), F32), [VMEM, VMEM, SMEM] + [VMEM] * 8, VMEM,
        [pltpu.VMEM((16, LANE), F32)],
    )(mlp_bias, mlp_out, out_bias, *near(*ha, *hb))


def shift(v, axis, size, k):
    return lax.ppermute(v, axis, [(i, (i + k) % size) for i in range(size)])


def spread(v, axis, size):
    out = [v]
    for k in range(1, size):
        out.append(shift(v, axis, size, size - k))
    return out


def around(v):
    half = NZ // 2
    after = shift(v, "y", NY, NY - 1)
    before = shift(v, "y", NY, 1)
    first = shift(after[:half], "y", NY, NY - 1)
    second = shift(before[half:], "y", NY, 1)
    return [v, after, before, first, second]


def deal(parts):
    out = [parts[0]]
    for k in range(1, NX):
        out.append(shift(parts[k], "x", NX, k))
    return out


def exchange(v, axis):
    return lax.all_to_all(v, axis, 0, 0, tiled=True)


def swaps(vs):
    return [shift(v, "c", NC, 1) for v in vs]


def tie(v, *others):
    return lax.optimization_barrier((v, *others))[0]


def on_device(
    cache, backing, resident, promote, victim, lookups, route,
    dcn_down, dcn_up, dcn_bias, mlp_in, mlp_bias, mlp_out, out_bias,
):
    cache = cache[0]
    backing = backing[0]
    bias = dcn_bias.reshape(-1, E)
    outgoing = fetch(promote, victim, backing)
    arrived = exchange(outgoing, ("y", "c"))
    wanted = jnp.transpose(lookups[:, :, 0, :], (0, 2, 1))
    sent, factors = route_lookups(wanted, route[:, 0].reshape(2, -1, LANE), dcn_down)
    piece = make_piece(victim, arrived, cache, factors, sent)
    mixed = exchange(piece, "z")
    top = own_weights(dcn_up, mlp_in)
    own = spread(mixed[:, :160, :], "y", NY)
    mixed = mixed[:, 160:, :]
    tops = stacked(spread(tie(top, piece), "z", NZ))
    tables = own + swaps(own)
    own = around(tops)
    tops = own + swaps(own)
    x00, low0, table, factors, new_cache = pool0(mixed, tables)
    lows0 = spread(low0, "x", NX)
    x01, low1 = pool1(tie(mixed, low0, bias), table, factors)
    lows1 = spread(low1, "x", NX)
    h0 = cross(lows0, bias, tops, tie(x00, low1))
    ra = deal(h0)
    h1 = cross(lows1, bias, tops, tie(x01, h0[0]))
    rb = deal(h1)
    new_backing = write_back(resident, victim, cache, tie(backing, h1[0]))
    scores = score(mlp_bias.reshape(8, LANE), mlp_out.reshape(8, LANE), out_bias, ra, rb)
    return scores[:, None, :], new_cache[None], new_backing[None]


def solution(mesh):
    fine = Mesh(mesh.devices.reshape(NX, NZ, NY, NC), ("x", "z", "y", "c"))
    ca, ow = ("x", "z"), ("y", "c")
    in_specs = (
        P(ca, None, None, None),
        P(ca, ow, None, None),
        P(ca, None),
        P(ca, None),
        P(ca, None),
        P(None, ow, ca, None),
        P(None, ow, None),
        P(ca, None),
        P(None, ca),
        P(),
        P(ca, None),
        P(),
        P(),
        P(),
    )
    out_specs = (
        P(None, ow, ca),
        P(ca, None, None, None),
        P(ca, ow, None, None),
    )
    return jax.shard_map(
        on_device, mesh=fine, in_specs=in_specs, out_specs=out_specs, check_vma=False
    )
```
